32 devices in a mesh: grp: 4 (over x, core), tile: 8 (over z, y).
Axes of the slice: x: 2, y: 2, z: 4, core: 2. Of those that a mesh axis runs over, the one named last changes fastest.
Arguments:
- flow_state: float32 [4, 4, 32, 2048], P('grp', None, 'tile'), may hold values from -6 to 6
- line_owner: int32 [8192, 1], replicated, may hold values from 0 to 7; in each aligned block of 8192 rows (0 to 8191, 8192 to 16383, ...) at most 2048 rows name the same one
Outputs:
- record: float32 [4, 8, 32, 2048], P('grp', 'tile')
The draws below stay inside these ranges and needn't reach their ends.
Inputs may be any that keep to these rules, and one draw needn't show every extreme that they name: `line_owner`: no pencil owns more than 2048 lines, some pencil owns exactly 2048, and every pencil owns at least one line.
All inputs are finite; a program needn't handle non-finite values.
Results may differ from the reference program's by a relative error of at most 0.00002.
Values sent between devices are 32-bit elements; how exact they have to be, the bound alone decides.
A program may use at most 64 MiB of HBM per device.

```python
import math
import jax
import jax.numpy as jnp
import numpy as np
from jax import lax

NY = 2048
PLANES = 4
NX = 32
NL = 8192
CAP = 2048
N_GRP = 4
N_TILE = 8


def steps_of(rng, shape, shards, least, largest):
    loudness, own = 1.0, jax.random.fold_in(rng, 6)
    for dim, parts in shards:
        steps = jnp.exp(jax.random.uniform(jax.random.fold_in(own, dim), (parts,), jnp.float32, least / len(shards), largest / len(shards)))
        loudness = loudness * jnp.repeat(steps, shape[dim] // parts).reshape([-1 if axis == dim else 1 for axis in range(len(shape))])
    return loudness


def assign_block(rng, own, number, rows, amount, top, limit, skew):
    ranking = jax.random.permutation(rng, amount)
    crowded, ordinary = portions_of(amount, rows * top, limit, skew, True), portions_of(amount, rows * top, limit, skew, False)
    places = jnp.arange(amount)

    def named(tallies, offset_by):
        used = int((tallies > 0).sum())
        fixed = max(1, used // 4)
        moved = fixed + (places - fixed + offset_by * (used - fixed)) % max(1, amount - fixed)
        return jnp.zeros((amount,), jnp.int32).at[ranking[jnp.where(places < fixed, places, moved)]].set(jnp.asarray(tallies, jnp.int32))

    tallies = jnp.where(number % 4 == 0, named(crowded, number // 4), named(ordinary, number - number // 4 - 1))
    mixed = jax.random.permutation(jax.random.fold_in(own, 3), amount)
    giver, receiver = mixed[0:amount // 2 * 2:2], mixed[1:amount // 2 * 2:2]
    room = jnp.minimum(tallies[giver] - 1, limit - tallies[receiver]) // 2
    room = jnp.where((giver == ranking[0]) | (receiver == ranking[0]) | (tallies[receiver] == 0), 0, jnp.maximum(room, 0))
    moved = jax.random.randint(jax.random.fold_in(own, 4), (amount // 2,), 0, 1 << 20) % (room + 1)
    tallies = tallies.at[giver].add(-moved).at[receiver].add(moved)
    labels = jnp.searchsorted(jnp.cumsum(tallies), jnp.arange(rows * top), side="right").astype(jnp.int32)
    listing = labels.reshape(top, rows).T
    listing = listing[jax.random.permutation(jax.random.fold_in(own, 1), rows)]
    offset_by = jax.random.randint(jax.random.fold_in(own, 2), (rows, 1), 0, top)
    return jnp.take_along_axis(listing, (jnp.arange(top)[None, :] + offset_by) % top, axis=1)


def portions_of(count, total, bound, lean, full):
    loads = [(1 << 20) // math.isqrt(grade ** lean) + 1 for grade in range(1, count + 1)]
    largest = bound if full else min(bound, max(-(-total // count), total * loads[0] // sum(loads)))
    least = 1 if total - largest >= count - 1 else 0
    holding, rest = [largest] + [least] * (count - 1), total - largest - least * (count - 1)
    while rest > 0:
        movable = [i for i in range(1, count) if holding[i] < largest] or [i for i in range(1, count) if holding[i] < bound]
        pool, remaining = sum([loads[i] for i in movable]), rest
        for i in movable:
            addition = min(bound - holding[i], max(1, remaining * loads[i] // pool), rest)
            holding[i] = holding[i] + addition
            rest = rest - addition
    return np.array(holding)


def centred(key, dims, scale, reach, pieces=(), kind=jnp.bfloat16):
    factor_of = steps_of(key, dims, pieces, -0.22, 0.18) if pieces else 1.0
    array = jax.random.normal(key, dims, jnp.float32) * scale * factor_of
    return jnp.minimum(jnp.maximum(array, -reach), reach).astype(kind)


def setup_inputs(seed: int = 0) -> dict:
    key_list = jax.random.split(jax.random.key(seed), 3)
    flow_state = centred(key_list[0], (N_GRP, PLANES, NX, NY), 1.0, 6.0, ((0, 4), (2, 8)), jnp.float32)
    line_owner_keys = jax.random.split(jax.random.fold_in(key_list[1], 1), NL // NL)
    line_owner_turns = jax.random.permutation(jax.random.fold_in(key_list[1], 3), NL // NL)
    line_owner = jax.vmap(lambda own, number: assign_block(jax.random.fold_in(key_list[1], 2), own, number, NL, N_TILE, 1, CAP, 2))(line_owner_keys, line_owner_turns).reshape((NL, 1))
    return {"flow_state": flow_state, "line_owner": line_owner}


time_step = 0.2
viscosity = 0.05
first_coeffs = (0.8, -0.2, 4.0 / 105.0, -1.0 / 280.0)
second_center = -205.0 / 72.0
second_coeffs = (1.6, -0.2, 8.0 / 315.0, -1.0 / 560.0)
lift_alpha = -1.586134342059924
lift_beta = -0.052980118572961
lift_gamma = 0.882911075530934
lift_delta = 0.443506852043971
lift_scale = 1.149604398860241


def first_rolled(field_now, along_axis):
    running = jnp.zeros_like(field_now)
    for offset in range(4):
        forward = jnp.roll(field_now, -(offset + 1), along_axis)
        behind = jnp.roll(field_now, offset + 1, along_axis)
        running = running + first_coeffs[offset] * (forward - behind)
    return running


def second_rolled(field_now, along_axis):
    running = second_center * field_now
    for offset in range(4):
        forward = jnp.roll(field_now, -(offset + 1), along_axis)
        behind = jnp.roll(field_now, offset + 1, along_axis)
        running = running + second_coeffs[offset] * (forward + behind)
    return running


def tendencies(fields):
    pressure = fields[3]
    grad_axes = (1, 2, 0)
    result = []
    for component in range(3):
        field_now = fields[component]
        advect = fields[0] * first_rolled(field_now, 1) + fields[1] * first_rolled(field_now, 2) + fields[2] * first_rolled(field_now, 0)
        laplace = second_rolled(field_now, 1) + second_rolled(field_now, 2) + second_rolled(field_now, 0)
        result.append(-advect - first_rolled(pressure, grad_axes[component]) + viscosity * laplace)
    return jnp.stack(result)


def lift_axis(signal, along_axis):
    length = signal.shape[along_axis]
    even_part = lax.slice_in_dim(signal, 0, length, 2, along_axis)
    odd_part = lax.slice_in_dim(signal, 1, length, 2, along_axis)
    odd_part = odd_part + lift_alpha * (even_part + jnp.roll(even_part, -1, along_axis))
    even_part = even_part + lift_beta * (odd_part + jnp.roll(odd_part, 1, along_axis))
    odd_part = odd_part + lift_gamma * (even_part + jnp.roll(even_part, -1, along_axis))
    even_part = even_part + lift_delta * (odd_part + jnp.roll(odd_part, 1, along_axis))
    return jnp.concatenate([even_part * lift_scale, odd_part / lift_scale], along_axis)


def line_slots(line_owner, pencils, capacity):
    owners = line_owner[:, 0].astype(jnp.int32)
    sorted_lines = jnp.argsort(owners, stable=True).astype(jnp.int32)
    sorted_owner = owners[sorted_lines]
    targets = jnp.arange(pencils, dtype=jnp.int32)
    starts = jnp.searchsorted(sorted_owner, targets, side="left").astype(jnp.int32)
    ends_at = jnp.searchsorted(sorted_owner, targets, side="right").astype(jnp.int32)
    counts = ends_at - starts
    slot_index = jnp.arange(capacity, dtype=jnp.int32)
    position = jnp.minimum(starts[:, None] + slot_index[None, :], owners.shape[0] - 1)
    chosen = sorted_lines[position]
    usable = slot_index[None, :] < counts[:, None]
    return chosen, usable


def reference(flow_state, line_owner):
    velocity = flow_state[:3]
    pressure = flow_state[3:]
    middle = velocity + time_step * tendencies(flow_state)
    finished = 0.5 * ((velocity + middle) + time_step * tendencies(jnp.concatenate([middle, pressure], 0)))
    coeffs = lift_axis(lift_axis(lift_axis(finished, 3), 1), 2)
    planes = coeffs.shape[1]
    line_table = jnp.transpose(coeffs, (0, 1, 3, 2)).reshape(3, planes * coeffs.shape[3], coeffs.shape[2])
    chosen, usable = line_slots(line_owner, N_TILE, CAP)
    picked = jnp.take(line_table, chosen.reshape(-1), axis=1).reshape(3, N_TILE, CAP, line_table.shape[2])
    picked = jnp.where(usable[None, :, :, None], picked, 0.0)
    record = jnp.transpose(picked, (0, 1, 3, 2))
    energy = record[0] * record[0] + record[1] * record[1] + record[2] * record[2]
    return jnp.concatenate([record, energy[None]], 0)
```

```python
import functools

import jax
import jax.numpy as jnp
import numpy as np
from jax import lax
from jax.experimental import pallas as pl
from jax.experimental.pallas import tpu as pltpu
from jax.sharding import PartitionSpec as P

time_step = 0.2
viscosity = 0.05
reach = 4
first_coeffs = (0.8, -0.2, 4.0 / 105.0, -1.0 / 280.0)
second_center = -205.0 / 72.0
second_coeffs = (1.6, -0.2, 8.0 / 315.0, -1.0 / 560.0)
lift_alpha = -1.586134342059924
lift_beta = -0.052980118572961
lift_gamma = 0.882911075530934
lift_delta = 0.443506852043971
lift_scale = 1.149604398860241
LANES = 128
MESH = pl.DeviceIdType.MESH


def lift_numpy(signal):
    even, odd = signal[0::2].copy(), signal[1::2].copy()
    odd += lift_alpha * (even + np.roll(even, -1, 0))
    even += lift_beta * (odd + np.roll(odd, 1, 0))
    odd += lift_gamma * (even + np.roll(even, -1, 0))
    even += lift_delta * (odd + np.roll(odd, 1, 0))
    return np.concatenate([even * lift_scale, odd / lift_scale])


def lift_matrix(length):
    return lift_numpy(np.eye(length))


def band_matrix():
    full = lift_matrix(8 * LANES)
    low = full[LANES : 2 * LANES, LANES : 5 * LANES]
    high = full[4 * LANES + LANES : 4 * LANES + 2 * LANES, LANES : 5 * LANES]
    return np.concatenate([low, high]).T.astype(np.float32)


def shifted_y(value, k):
    return pltpu.roll(value, (-k) % value.shape[-1], value.ndim - 1)


def derivatives(center, shift, want_first=True, want_second=True):
    first, second = None, second_center * center if want_second else None
    for k in range(1, reach + 1):
        ahead, behind = shift(k), shift(-k)
        if want_first:
            term = first_coeffs[k - 1] * (ahead - behind)
            first = term if first is None else first + term
        if want_second:
            second = second + second_coeffs[k - 1] * (ahead + behind)
    return first, second


def flow_kernel(n_tile, own_ref, band_ref, out_ref, fields, mids, halo, mid_halo, pad, ppad, middle, fin,
                send_sem, recv_sem, hsend_sem, hrecv_sem, msend_sem, mrecv_sem, mhsend_sem, mhrecv_sem):
    g, t = lax.axis_index("grp"), lax.axis_index("tile")
    right, left = lax.rem(t + 1, n_tile), lax.rem(t + n_tile - 1, n_tile)
    planes, rows, ny = own_ref.shape[1:]
    own = own_ref.at[0]

    def gather_copy(src, dst, ssem, rsem, k, slot):
        return pltpu.make_async_remote_copy(
            src_ref=src, dst_ref=dst.at[slot], send_sem=ssem.at[k], recv_sem=rsem.at[slot],
            device_id=(k, t), device_id_type=MESH)

    def halo_copy(src, dst, ssem, rsem, side, slot, group):
        return pltpu.make_async_remote_copy(
            src_ref=src, dst_ref=dst.at[slot + side], send_sem=ssem.at[side], recv_sem=rsem.at[slot + side],
            device_id=(group, right if side == 0 else left), device_id_type=MESH)

    @pl.when(g < 3)
    def _():
        for side in range(2):
            halo_copy(own, halo, hsend_sem, hrecv_sem, side, 0, g).start()

    for k in range(3):
        @pl.when(g != k)
        def _(k=k):
            gather_copy(own, fields, send_sem, recv_sem, k, g).start()

    @pl.when(g == 3)
    def _():
        for side in range(2):
            halo_copy(own, halo, hsend_sem, hrecv_sem, side, 2, 0).start()

    @pl.when(g < 3)
    def _():
        for k in range(3):
            @pl.when(g == k)
            def _(k=k):
                fields[k] = own_ref[0]

        for z in range(planes):
            pad[z, reach : reach + rows] = own_ref[0, z]

        for k in range(4):
            @pl.when(g != k)
            def _(k=k):
                gather_copy(own, fields, send_sem, recv_sem, 0, k).wait_recv()
        for side in range(2):
            halo_copy(own, halo, hsend_sem, hrecv_sem, side, 0, g).wait_recv()

        @pl.when(g == 0)
        def _():
            for side in range(2):
                halo_copy(own, halo, hsend_sem, hrecv_sem, side, 2, 0).wait_recv()
            for z in range(planes):
                ppad[z, 0:reach] = halo[2, z, rows - reach : rows]
                ppad[z, reach : reach + rows] = fields[3, z]
                ppad[z, reach + rows : 2 * reach + rows] = halo[3, z, 0:reach]
            for z in range(planes):
                middle[z], _ = derivatives(None, lambda k: ppad[z, reach + k : reach + k + rows], True, False)

        @pl.when(g == 1)
        def _():
            for z in range(planes):
                value = fields[3, z]
                middle[z], _ = derivatives(None, lambda k: shifted_y(value, k), True, False)

        @pl.when(g == 2)
        def _():
            for z in range(planes):
                middle[z], _ = derivatives(None, lambda k: fields[3, (z + k) % planes], True, False)

        def tendency(z, vel, press):
            center = pad[z, reach : reach + rows]
            fx, sx = derivatives(center, lambda k: pad[z, reach + k : reach + k + rows])
            fy, sy = derivatives(center, lambda k: shifted_y(center, k))
            fz, sz = derivatives(center, lambda k: pad[(z + k) % planes, reach : reach + rows])
            advect = vel[0, z] * fx + vel[1, z] * fy + vel[2, z] * fz
            return viscosity * (sx + sy + sz) - advect - press

        for z in range(planes):
            pad[z, 0:reach] = halo[0, z, rows - reach : rows]
            pad[z, reach + rows : 2 * reach + rows] = halo[1, z, 0:reach]
        for z in range(planes):
            press = middle[z]
            ppad[z, 0:rows] = press
        for z in range(planes):
            middle[z] = own_ref[0, z] + time_step * tendency(z, fields, ppad[z, 0:rows])

        for side in range(2):
            halo_copy(middle, mid_halo, mhsend_sem, mhrecv_sem, side, 0, g).start()
        for k in range(3):
            @pl.when(g != k)
            def _(k=k):
                gather_copy(middle, mids, msend_sem, mrecv_sem, k, g).start()

            @pl.when(g == k)
            def _(k=k):
                mids[k] = middle[...]

        for z in range(planes):
            pad[z, reach : reach + rows] = middle[z]
        for k in range(3):
            @pl.when(g != k)
            def _(k=k):
                gather_copy(middle, mids, msend_sem, mrecv_sem, 0, k).wait_recv()
        for side in range(2):
            halo_copy(middle, mid_halo, mhsend_sem, mhrecv_sem, side, 0, g).wait_recv()
        for z in range(planes):
            pad[z, 0:reach] = mid_halo[0, z, rows - reach : rows]
            pad[z, reach + rows : 2 * reach + rows] = mid_halo[1, z, 0:reach]
        for z in range(planes):
            fin[z] = 0.5 * ((own_ref[0, z] + middle[z]) + time_step * tendency(z, mids, ppad[z, 0:rows]))

        blocks = ny // (2 * LANES)
        groups = ny // LANES
        for z in range(planes):
            value = fin[z]
            pieces = []
            for b in range(blocks):
                window = [value[:, ((2 * b + j) % groups) * LANES : ((2 * b + j) % groups + 1) * LANES] for j in (-1, 0, 1, 2)]
                pieces.append(jnp.concatenate(window, axis=1))
            stacked = jnp.concatenate(pieces, axis=0)
            lifted = jnp.dot(stacked, band_ref[...], precision=lax.Precision.HIGHEST, preferred_element_type=jnp.float32)
            for b in range(blocks):
                piece = lifted[b * rows : (b + 1) * rows]
                fin[z, :, b * LANES : (b + 1) * LANES] = piece[:, 0:LANES]
                fin[z, :, ny // 2 + b * LANES : ny // 2 + (b + 1) * LANES] = piece[:, LANES:]

        half = planes // 2
        even = [fin[2 * i] for i in range(half)]
        odd = [fin[2 * i + 1] for i in range(half)]
        odd = [odd[i] + lift_alpha * (even[i] + even[(i + 1) % half]) for i in range(half)]
        even = [even[i] + lift_beta * (odd[i] + odd[(i - 1) % half]) for i in range(half)]
        odd = [odd[i] + lift_gamma * (even[i] + even[(i + 1) % half]) for i in range(half)]
        even = [even[i] + lift_delta * (odd[i] + odd[(i - 1) % half]) for i in range(half)]
        for i in range(half):
            out_ref[i] = even[i] * lift_scale
            out_ref[half + i] = odd[i] * (1.0 / lift_scale)

        for side in range(2):
            halo_copy(middle, mid_halo, mhsend_sem, mhrecv_sem, side, 0, g).wait_send()
        for k in range(3):
            @pl.when(g != k)
            def _(k=k):
                gather_copy(middle, mids, msend_sem, mrecv_sem, k, g).wait_send()

    @pl.when(g == 3)
    def _():
        out_ref[...] = jnp.zeros_like(out_ref)

    for side in range(2):
        halo_copy(own, halo, hsend_sem, hrecv_sem, side, 0, g).wait_send()
    for k in range(3):
        @pl.when(g != k)
        def _(k=k):
            gather_copy(own, fields, send_sem, recv_sem, k, g).wait_send()


def slots_kernel(n_tile, owner_ref, place_ref, base_ref, count_ref):
    owner = owner_ref[...]
    n_blocks = owner.shape[0]
    upper = (lax.broadcasted_iota(jnp.int32, (LANES, LANES), 0) <= lax.broadcasted_iota(jnp.int32, (LANES, LANES), 1)).astype(jnp.float32)
    lower = (lax.broadcasted_iota(jnp.int32, (n_blocks, n_blocks), 0) > lax.broadcasted_iota(jnp.int32, (n_blocks, n_blocks), 1)).astype(jnp.float32)
    lane = lax.broadcasted_iota(jnp.int32, (n_blocks, LANES), 1)

    def step(s, carry):
        place, counts, ahead = carry
        mask = (owner == s).astype(jnp.float32)
        within = jnp.dot(mask, upper, preferred_element_type=jnp.float32)
        total = jnp.sum(mask, axis=1, keepdims=True)
        place = place + mask * (ahead + within - 1.0)
        counts = jnp.where(lane == s, total, counts)
        return place, counts, ahead + total

    zeros = jnp.zeros((n_blocks, LANES), jnp.float32)
    carry = (zeros, zeros, jnp.zeros((n_blocks, 1), jnp.float32))
    if n_tile <= 16:
        for s in range(n_tile):
            carry = step(s, carry)
    else:
        carry = lax.fori_loop(0, n_tile, step, carry)
    place, counts, _ = carry
    place_ref[...] = place
    count_ref[...] = counts.astype(jnp.int32)
    base_ref[...] = jnp.dot(lower, counts, preferred_element_type=jnp.float32).astype(jnp.int32)


def compact_kernel(n_tile, base_ref, count_ref, coeff_ref, place_ref, out_ref, current):
    planes, rows, ny = coeff_ref.shape
    groups = ny // LANES
    out_ref[...] = jnp.zeros_like(out_ref)
    current[...] = jnp.zeros_like(current)
    rank = lax.broadcasted_iota(jnp.int32, (LANES, LANES), 0).astype(jnp.float32)
    lane = lax.broadcasted_iota(jnp.int32, (rows, LANES), 1)

    def block(b, _):
        z, y = b // groups, b % groups
        value = coeff_ref[z, :, pl.ds(pl.multiple_of(y * LANES, LANES), LANES)]
        high = value.astype(jnp.bfloat16).astype(jnp.float32)
        rest = value - high
        mid = rest.astype(jnp.bfloat16).astype(jnp.float32)
        low = rest - mid
        parts = jnp.concatenate([high, mid, low], axis=0).astype(jnp.bfloat16)
        chosen = jnp.where(rank == place_ref[pl.ds(b, 1), :], 1.0, 0.0).astype(jnp.bfloat16)
        ordered = lax.dot_general(parts, chosen, (((1,), (1,)), ((), ())), preferred_element_type=jnp.float32)
        ordered = (ordered[0:rows] + ordered[rows : 2 * rows]) + ordered[2 * rows : 3 * rows]

        def pencil(s, ahead):
            base, count = base_ref[b, s], count_ref[b, s]
            start = base & (LANES - 1)
            end = start + count
            turned = pltpu.roll(ordered, (start - ahead) & (LANES - 1), 1)
            now = current[s] + jnp.where((lane >= start) & (lane < end), turned, 0.0)
            group = pl.multiple_of(base - start, LANES)
            out_ref[s, :, pl.ds(group, LANES)] = now
            after = jnp.where(lane < end - LANES, turned, 0.0)
            keep = jnp.where(end >= LANES, after, now)
            current[s] = keep
            out_ref[s, :, pl.ds(group + LANES, LANES)] = after
            return ahead + count

        if n_tile <= 16:
            ahead = jnp.int32(0)
            for s in range(n_tile):
                ahead = pencil(s, ahead)
        else:
            lax.fori_loop(0, n_tile, pencil, jnp.int32(0))
        return 0

    lax.fori_loop(0, planes * groups, block, 0)


def record_kernel(n_tile, chunks, sent_ref, matrix_ref, out_ref, got, records, send_sem, recv_sem, rsend_sem, rrecv_sem):
    g, t = lax.axis_index("grp"), lax.axis_index("tile")
    rows, nx, cap = sent_ref.shape[1], out_ref.shape[0], out_ref.shape[1]
    width = cap // chunks

    def exchange(s, slot):
        return pltpu.make_async_remote_copy(
            src_ref=sent_ref.at[s, :, pl.ds(0, cap)], dst_ref=got.at[slot], send_sem=send_sem.at[s],
            recv_sem=recv_sem.at[slot], device_id=(g, s), device_id_type=MESH)

    def report(c, slot):
        part = pl.ds(c * width, width)
        return pltpu.make_async_remote_copy(
            src_ref=out_ref.at[:, part], dst_ref=records.at[slot, :, part], send_sem=rsend_sem.at[c],
            recv_sem=rrecv_sem.at[slot, c], device_id=(3, t), device_id_type=MESH)

    @pl.when(g < 3)
    def _():
        for k in range(1, n_tile):
            exchange(lax.rem(t + k, n_tile), t).start()
        got[t] = sent_ref[t, :, 0:cap]
        for k in range(1, n_tile):
            exchange(lax.rem(t + k, n_tile), lax.rem(t + k, n_tile)).wait_recv()
        matrix = matrix_ref[...]
        for c in range(chunks):
            value = got[:, :, c * width : (c + 1) * width].reshape(nx, width)
            out_ref[:, c * width : (c + 1) * width] = jnp.dot(
                matrix, value, precision=lax.Precision.HIGHEST, preferred_element_type=jnp.float32)
            report(c, g).start()
        for k in range(1, n_tile):
            exchange(lax.rem(t + k, n_tile), t).wait_send()
        for c in range(chunks):
            report(c, g).wait_send()

    @pl.when(g == 3)
    def _():
        for c in range(chunks):
            for k in range(3):
                report(c, k).wait_recv()
            part = slice(c * width, (c + 1) * width)
            first, second, third = records[0, :, part], records[1, :, part], records[2, :, part]
            out_ref[:, part] = first * first + second * second + third * third


def body(flow_state, line_owner, *, n_tile):
    _, planes, rows, ny = flow_state.shape
    n_lines = line_owner.shape[0]
    n_blocks = n_lines // LANES
    nx = rows * n_tile
    cap = 2 * planes * ny // n_tile
    vmem = pl.BlockSpec(memory_space=pltpu.VMEM)
    smem = pl.BlockSpec(memory_space=pltpu.SMEM)
    f32 = jnp.float32
    shape = jax.ShapeDtypeStruct
    limit = 56 * 1024 * 1024
    dma = pltpu.SemaphoreType.DMA
    owner = line_owner.reshape(n_blocks, LANES)
    place, base, count = pl.pallas_call(
        functools.partial(slots_kernel, n_tile),
        out_shape=(shape((n_blocks, LANES), f32), shape((n_blocks, LANES), jnp.int32), shape((n_blocks, LANES), jnp.int32)),
        in_specs=[vmem], out_specs=(vmem, vmem, vmem), name="slots",
    )(owner)
    tile = (planes, rows, ny)
    coeffs = pl.pallas_call(
        functools.partial(flow_kernel, n_tile),
        out_shape=shape(tile, f32),
        in_specs=[vmem, vmem], out_specs=vmem,
        scratch_shapes=[
            pltpu.VMEM((4,) + tile, f32), pltpu.VMEM((3,) + tile, f32),
            pltpu.VMEM((4,) + tile, f32), pltpu.VMEM((2,) + tile, f32),
            pltpu.VMEM((planes, rows + 2 * reach, ny), f32), pltpu.VMEM((planes, rows + 2 * reach, ny), f32),
            pltpu.VMEM(tile, f32), pltpu.VMEM(tile, f32),
            dma((4,)), dma((4,)), dma((2,)), dma((4,)), dma((4,)), dma((4,)), dma((2,)), dma((2,)),
        ],
        compiler_params=pltpu.CompilerParams(has_side_effects=True, vmem_limit_bytes=limit), name="flow",
    )(flow_state, jnp.asarray(band_matrix()))
    sent = pl.pallas_call(
        functools.partial(compact_kernel, n_tile),
        out_shape=shape((n_tile, rows, cap + 2 * LANES), f32),
        in_specs=[smem, smem, vmem, vmem], out_specs=vmem,
        scratch_shapes=[pltpu.VMEM((n_tile, rows, LANES), f32)],
        compiler_params=pltpu.CompilerParams(vmem_limit_bytes=limit), name="compact",
    )(base, count, coeffs, place)
    chunks = 4 if cap % (4 * LANES) == 0 else 1
    record = pl.pallas_call(
        functools.partial(record_kernel, n_tile, chunks),
        out_shape=shape((nx, cap), f32),
        in_specs=[vmem, vmem], out_specs=vmem,
        scratch_shapes=[
            pltpu.VMEM((n_tile, rows, cap), f32), pltpu.VMEM((3, nx, cap), f32),
            dma((n_tile,)), dma((n_tile,)), dma((chunks,)), dma((3, chunks)),
        ],
        compiler_params=pltpu.CompilerParams(has_side_effects=True, vmem_limit_bytes=limit), name="record",
    )(sent, jnp.asarray(lift_matrix(nx).astype(np.float32)))
    return record[None, None]


def solution(mesh):
    in_specs = (P("grp", None, "tile", None), P())
    out_specs = P("grp", "tile", None, None)
    run = functools.partial(body, n_tile=mesh.shape["tile"])
    return jax.shard_map(run, mesh=mesh, in_specs=in_specs, out_specs=out_specs, check_vma=False)
```

```python
import functools

import jax
import jax.numpy as jnp
import numpy as np
from jax import lax
from jax.experimental import pallas as pl
from jax.experimental.pallas import tpu as pltpu
from jax.sharding import PartitionSpec as P

time_step = 0.2
viscosity = 0.05
reach = 4
first_coeffs = (0.8, -0.2, 4.0 / 105.0, -1.0 / 280.0)
second_center = -205.0 / 72.0
second_coeffs = (1.6, -0.2, 8.0 / 315.0, -1.0 / 560.0)
lift_alpha = -1.586134342059924
lift_beta = -0.052980118572961
lift_gamma = 0.882911075530934
lift_delta = 0.443506852043971
lift_scale = 1.149604398860241
LANES = 128
MESH = pl.DeviceIdType.MESH


def lift_numpy(signal):
    even, odd = signal[0::2].copy(), signal[1::2].copy()
    odd += lift_alpha * (even + np.roll(even, -1, 0))
    even += lift_beta * (odd + np.roll(odd, 1, 0))
    odd += lift_gamma * (even + np.roll(even, -1, 0))
    even += lift_delta * (odd + np.roll(odd, 1, 0))
    return np.concatenate([even * lift_scale, odd / lift_scale])


def lift_matrix(length):
    return lift_numpy(np.eye(length))


def band_matrix():
    full = lift_matrix(8 * LANES)
    low = full[LANES : 2 * LANES, LANES : 5 * LANES]
    high = full[4 * LANES + LANES : 4 * LANES + 2 * LANES, LANES : 5 * LANES]
    return np.concatenate([low, high]).T.astype(np.float32)


def shifted_y(value, k):
    return pltpu.roll(value, (-k) % value.shape[-1], value.ndim - 1)


def derivatives(center, shift, want_first=True, want_second=True):
    first, second = None, second_center * center if want_second else None
    for k in range(1, reach + 1):
        ahead, behind = shift(k), shift(-k)
        if want_first:
            term = first_coeffs[k - 1] * (ahead - behind)
            first = term if first is None else first + term
        if want_second:
            second = second + second_coeffs[k - 1] * (ahead + behind)
    return first, second


def slots_of(n_tile, owner_ref, place_ref, base_ref, count_ref):
    owner = owner_ref[...]
    n_blocks = owner.shape[0]
    upper = (lax.broadcasted_iota(jnp.int32, (LANES, LANES), 0) <= lax.broadcasted_iota(jnp.int32, (LANES, LANES), 1)).astype(jnp.float32)
    lower = (lax.broadcasted_iota(jnp.int32, (n_blocks, n_blocks), 0) > lax.broadcasted_iota(jnp.int32, (n_blocks, n_blocks), 1)).astype(jnp.float32)
    lane = lax.broadcasted_iota(jnp.int32, (n_blocks, LANES), 1)

    def step(s, carry):
        place, counts, ahead = carry
        mask = (owner == s).astype(jnp.float32)
        within = jnp.dot(mask, upper, preferred_element_type=jnp.float32)
        total = jnp.sum(mask, axis=1, keepdims=True)
        place = place + mask * (ahead + within - 1.0)
        counts = jnp.where(lane == s, total, counts)
        return place, counts, ahead + total

    zeros = jnp.zeros((n_blocks, LANES), jnp.float32)
    carry = (zeros, zeros, jnp.zeros((n_blocks, 1), jnp.float32))
    if n_tile <= 16:
        for s in range(n_tile):
            carry = step(s, carry)
    else:
        carry = lax.fori_loop(0, n_tile, step, carry)
    place, counts, _ = carry
    place_ref[...] = place
    count_ref[...] = counts.astype(jnp.int32)
    base_ref[...] = jnp.dot(lower, counts, preferred_element_type=jnp.float32).astype(jnp.int32)


def flow_kernel(n_tile, own_ref, band_ref, owner_ref, out_ref, place_ref, base_ref, count_ref,
                fields, mids, halo, mid_halo, pad, ppad, middle, fin, along_y, along_z, lap, send_sem, recv_sem, hsend_sem, hrecv_sem, msend_sem, mrecv_sem, mhsend_sem, mhrecv_sem):
    g, t = lax.axis_index("grp"), lax.axis_index("tile")
    right, left = lax.rem(t + 1, n_tile), lax.rem(t + n_tile - 1, n_tile)
    planes, rows, ny = own_ref.shape[1:]
    own = own_ref.at[0]

    barrier = pltpu.get_barrier_semaphore()
    for k in range(1, 4):
        pl.semaphore_signal(barrier, inc=1, device_id=(lax.rem(g + k, 4), t), device_id_type=MESH)
    for side in (right, left):
        pl.semaphore_signal(barrier, inc=1, device_id=(g, side), device_id_type=MESH)

    @pl.when((g == 0) | (g == 3))
    def _():
        for side in (right, left):
            pl.semaphore_signal(barrier, inc=1, device_id=(3 - g, side), device_id_type=MESH)
        pl.semaphore_wait(barrier, 7)

    @pl.when((g == 1) | (g == 2))
    def _():
        pl.semaphore_wait(barrier, 5)

    def gather_copy(src, dst, ssem, rsem, k, slot):
        return pltpu.make_async_remote_copy(
            src_ref=src, dst_ref=dst.at[slot], send_sem=ssem.at[k], recv_sem=rsem.at[slot],
            device_id=(k, t), device_id_type=MESH)

    def halo_copy(src, dst, ssem, rsem, side, slot, group):
        return pltpu.make_async_remote_copy(
            src_ref=src, dst_ref=dst.at[slot + side], send_sem=ssem.at[side], recv_sem=rsem.at[slot + side],
            device_id=(group, right if side == 0 else left), device_id_type=MESH)

    @pl.when(g < 3)
    def _():
        for side in range(2):
            halo_copy(own, halo, hsend_sem, hrecv_sem, side, 0, g).start()

    for k in range(3):
        @pl.when(g != k)
        def _(k=k):
            gather_copy(own, fields, send_sem, recv_sem, k, g).start()

    @pl.when(g == 3)
    def _():
        for side in range(2):
            halo_copy(own, halo, hsend_sem, hrecv_sem, side, 2, 0).start()

    def local_terms():
        for z in range(planes):
            center = pad[z, reach : reach + rows]
            fy, sy = derivatives(center, lambda k: shifted_y(center, k))
            fz, sz = derivatives(center, lambda k: pad[(z + k) % planes, reach : reach + rows])
            along_y[z], along_z[z], lap[z] = fy, fz, sy + sz

    slots_of(n_tile, owner_ref, place_ref, base_ref, count_ref)

    @pl.when(g < 3)
    def _():
        for k in range(3):
            @pl.when(g == k)
            def _(k=k):
                fields[k] = own_ref[0]

        for z in range(planes):
            pad[z, reach : reach + rows] = own_ref[0, z]
        local_terms()

        for k in range(4):
            @pl.when(g != k)
            def _(k=k):
                gather_copy(own, fields, send_sem, recv_sem, 0, k).wait_recv()
        for side in range(2):
            halo_copy(own, halo, hsend_sem, hrecv_sem, side, 0, g).wait_recv()

        @pl.when(g == 0)
        def _():
            for side in range(2):
                halo_copy(own, halo, hsend_sem, hrecv_sem, side, 2, 0).wait_recv()
            for z in range(planes):
                ppad[z, 0:reach] = halo[2, z, rows - reach : rows]
                ppad[z, reach : reach + rows] = fields[3, z]
                ppad[z, reach + rows : 2 * reach + rows] = halo[3, z, 0:reach]
            for z in range(planes):
                middle[z], _ = derivatives(None, lambda k: ppad[z, reach + k : reach + k + rows], True, False)

        @pl.when(g == 1)
        def _():
            for z in range(planes):
                value = fields[3, z]
                middle[z], _ = derivatives(None, lambda k: shifted_y(value, k), True, False)

        @pl.when(g == 2)
        def _():
            for z in range(planes):
                middle[z], _ = derivatives(None, lambda k: fields[3, (z + k) % planes], True, False)

        def tendency(z, vel, press):
            center = pad[z, reach : reach + rows]
            fx, sx = derivatives(center, lambda k: pad[z, reach + k : reach + k + rows])
            advect = vel[0, z] * fx + vel[1, z] * along_y[z] + vel[2, z] * along_z[z]
            return viscosity * (sx + lap[z]) - advect - press

        for z in range(planes):
            pad[z, 0:reach] = halo[0, z, rows - reach : rows]
            pad[z, reach + rows : 2 * reach + rows] = halo[1, z, 0:reach]
        for z in range(planes):
            press = middle[z]
            ppad[z, 0:rows] = press
        for z in range(planes):
            middle[z] = own_ref[0, z] + time_step * tendency(z, fields, ppad[z, 0:rows])

        for side in range(2):
            halo_copy(middle, mid_halo, mhsend_sem, mhrecv_sem, side, 0, g).start()
        for k in range(3):
            @pl.when(g != k)
            def _(k=k):
                gather_copy(middle, mids, msend_sem, mrecv_sem, k, g).start()

            @pl.when(g == k)
            def _(k=k):
                mids[k] = middle[...]

        for z in range(planes):
            pad[z, reach : reach + rows] = middle[z]
        local_terms()
        for k in range(3):
            @pl.when(g != k)
            def _(k=k):
                gather_copy(middle, mids, msend_sem, mrecv_sem, 0, k).wait_recv()
        for side in range(2):
            halo_copy(middle, mid_halo, mhsend_sem, mhrecv_sem, side, 0, g).wait_recv()
        for z in range(planes):
            pad[z, 0:reach] = mid_halo[0, z, rows - reach : rows]
            pad[z, reach + rows : 2 * reach + rows] = mid_halo[1, z, 0:reach]
        for z in range(planes):
            fin[z] = 0.5 * ((own_ref[0, z] + middle[z]) + time_step * tendency(z, mids, ppad[z, 0:rows]))

        blocks = ny // (2 * LANES)
        groups = ny // LANES
        for z in range(planes):
            value = fin[z]
            pieces = []
            for b in range(blocks):
                window = [value[:, ((2 * b + j) % groups) * LANES : ((2 * b + j) % groups + 1) * LANES] for j in (-1, 0, 1, 2)]
                pieces.append(jnp.concatenate(window, axis=1))
            stacked = jnp.concatenate(pieces, axis=0)
            lifted = jnp.dot(stacked, band_ref[...], precision=lax.Precision.HIGHEST, preferred_element_type=jnp.float32)
            for b in range(blocks):
                piece = lifted[b * rows : (b + 1) * rows]
                fin[z, :, b * LANES : (b + 1) * LANES] = piece[:, 0:LANES]
                fin[z, :, ny // 2 + b * LANES : ny // 2 + (b + 1) * LANES] = piece[:, LANES:]

        half = planes // 2
        even = [fin[2 * i] for i in range(half)]
        odd = [fin[2 * i + 1] for i in range(half)]
        odd = [odd[i] + lift_alpha * (even[i] + even[(i + 1) % half]) for i in range(half)]
        even = [even[i] + lift_beta * (odd[i] + odd[(i - 1) % half]) for i in range(half)]
        odd = [odd[i] + lift_gamma * (even[i] + even[(i + 1) % half]) for i in range(half)]
        even = [even[i] + lift_delta * (odd[i] + odd[(i - 1) % half]) for i in range(half)]
        for i in range(half):
            out_ref[i] = even[i] * lift_scale
            out_ref[half + i] = odd[i] * (1.0 / lift_scale)

        for side in range(2):
            halo_copy(middle, mid_halo, mhsend_sem, mhrecv_sem, side, 0, g).wait_send()
        for k in range(3):
            @pl.when(g != k)
            def _(k=k):
                gather_copy(middle, mids, msend_sem, mrecv_sem, k, g).wait_send()

    @pl.when(g == 3)
    def _():
        out_ref[...] = jnp.zeros_like(out_ref)

    for side in range(2):
        halo_copy(own, halo, hsend_sem, hrecv_sem, side, 0, g).wait_send()
    for k in range(3):
        @pl.when(g != k)
        def _(k=k):
            gather_copy(own, fields, send_sem, recv_sem, k, g).wait_send()


def compact_kernel(n_tile, base_ref, count_ref, coeff_ref, place_ref, out_ref, current):
    planes, rows, ny = coeff_ref.shape
    groups = ny // LANES
    out_ref[...] = jnp.zeros_like(out_ref)
    current[...] = jnp.zeros_like(current)
    rank = lax.broadcasted_iota(jnp.int32, (LANES, LANES), 0).astype(jnp.float32)
    lane = lax.broadcasted_iota(jnp.int32, (rows, LANES), 1)

    def sort(b):
        z, y = b // groups, b % groups
        value = coeff_ref[z, :, pl.ds(pl.multiple_of(y * LANES, LANES), LANES)]
        high = value.astype(jnp.bfloat16).astype(jnp.float32)
        rest = value - high
        mid = rest.astype(jnp.bfloat16).astype(jnp.float32)
        low = rest - mid
        parts = jnp.concatenate([high, mid, low], axis=0).astype(jnp.bfloat16)
        chosen = jnp.where(rank == place_ref[pl.ds(b, 1), :], 1.0, 0.0).astype(jnp.bfloat16)
        ordered = lax.dot_general(parts, chosen, (((1,), (1,)), ((), ())), preferred_element_type=jnp.float32)
        return (ordered[0:rows] + ordered[rows : 2 * rows]) + ordered[2 * rows : 3 * rows]

    def pencil(b, ordered, s, ahead):
        base, count = base_ref[b, s], count_ref[b, s]
        start = base & (LANES - 1)
        end = start + count
        turned = pltpu.roll(ordered, (start - ahead) & (LANES - 1), 1)
        now = current[s] + jnp.where((lane >= start) & (lane < end), turned, 0.0)
        group = pl.multiple_of(base - start, LANES)
        after = jnp.where(lane < end - LANES, turned, 0.0)
        current[s] = jnp.where(end >= LANES, after, now)
        out_ref[s, :, pl.ds(group, 2 * LANES)] = jnp.concatenate([now, after], axis=1)
        return ahead + count

    n_blocks = planes * groups
    batch = 8 if n_blocks % 8 == 0 and n_tile <= 16 else 1

    def blocks(i, _):
        ordered = [sort(i * batch + j) for j in range(batch)]
        for j in range(batch):
            b = i * batch + j
            if n_tile <= 16:
                ahead = jnp.int32(0)
                for s in range(n_tile):
                    ahead = pencil(b, ordered[j], s, ahead)
            else:
                lax.fori_loop(0, n_tile, lambda s, ahead: pencil(b, ordered[j], s, ahead), jnp.int32(0))
        return 0

    lax.fori_loop(0, n_blocks // batch, blocks, 0)


def record_kernel(n_tile, chunks, sent_ref, matrix_ref, out_ref, got, records, send_sem, recv_sem, rsend_sem, rrecv_sem):
    g, t = lax.axis_index("grp"), lax.axis_index("tile")
    rows, nx, cap = sent_ref.shape[1], out_ref.shape[0], out_ref.shape[1]
    width = cap // chunks

    barrier = pltpu.get_barrier_semaphore()

    @pl.when(g < 3)
    def _():
        for k in range(1, n_tile):
            pl.semaphore_signal(barrier, inc=1, device_id=(g, lax.rem(t + k, n_tile)), device_id_type=MESH)
        pl.semaphore_signal(barrier, inc=1, device_id=(3, t), device_id_type=MESH)
        pl.semaphore_wait(barrier, n_tile)

    @pl.when(g == 3)
    def _():
        for k in range(3):
            pl.semaphore_signal(barrier, inc=1, device_id=(k, t), device_id_type=MESH)
        pl.semaphore_wait(barrier, 3)

    def exchange(s, slot, c):
        part = pl.ds(c * width, width)
        return pltpu.make_async_remote_copy(
            src_ref=sent_ref.at[s, :, part], dst_ref=got.at[slot, :, part], send_sem=send_sem.at[s, c],
            recv_sem=recv_sem.at[slot, c], device_id=(g, s), device_id_type=MESH)

    def report(c, slot):
        part = pl.ds(c * width, width)
        return pltpu.make_async_remote_copy(
            src_ref=out_ref.at[:, part], dst_ref=records.at[slot, :, part], send_sem=rsend_sem.at[c],
            recv_sem=rrecv_sem.at[slot, c], device_id=(3, t), device_id_type=MESH)

    @pl.when(g < 3)
    def _():
        for c in range(chunks):
            for k in range(1, n_tile):
                exchange(lax.rem(t + k, n_tile), t, c).start()
        got[t] = sent_ref[t, :, 0:cap]
        matrix = matrix_ref[...]
        for c in range(chunks):
            for k in range(1, n_tile):
                exchange(lax.rem(t + k, n_tile), lax.rem(t + k, n_tile), c).wait_recv()
            value = got[:, :, c * width : (c + 1) * width].reshape(nx, width)
            out_ref[:, c * width : (c + 1) * width] = jnp.dot(
                matrix, value, precision=lax.Precision.HIGHEST, preferred_element_type=jnp.float32)
            report(c, g).start()
        for c in range(chunks):
            for k in range(1, n_tile):
                exchange(lax.rem(t + k, n_tile), t, c).wait_send()
            report(c, g).wait_send()

    @pl.when(g == 3)
    def _():
        for c in range(chunks):
            for k in range(3):
                report(c, k).wait_recv()
            part = slice(c * width, (c + 1) * width)
            first, second, third = records[0, :, part], records[1, :, part], records[2, :, part]
            out_ref[:, part] = first * first + second * second + third * third


def body(flow_state, line_owner, *, n_tile):
    _, planes, rows, ny = flow_state.shape
    n_lines = line_owner.shape[0]
    n_blocks = n_lines // LANES
    nx = rows * n_tile
    cap = 2 * planes * ny // n_tile
    vmem = pl.BlockSpec(memory_space=pltpu.VMEM)
    smem = pl.BlockSpec(memory_space=pltpu.SMEM)
    f32 = jnp.float32
    shape = jax.ShapeDtypeStruct
    limit = 56 * 1024 * 1024
    dma = pltpu.SemaphoreType.DMA
    owner = line_owner.reshape(n_blocks, LANES)
    tile = (planes, rows, ny)
    ints = shape((n_blocks, LANES), jnp.int32)
    coeffs, place, base, count = pl.pallas_call(
        functools.partial(flow_kernel, n_tile),
        out_shape=(shape(tile, f32), shape((n_blocks, LANES), f32), ints, ints),
        in_specs=[vmem, vmem, vmem], out_specs=(vmem, vmem, vmem, vmem),
        scratch_shapes=[
            pltpu.VMEM((4,) + tile, f32), pltpu.VMEM((3,) + tile, f32),
            pltpu.VMEM((4,) + tile, f32), pltpu.VMEM((2,) + tile, f32),
            pltpu.VMEM((planes, rows + 2 * reach, ny), f32), pltpu.VMEM((planes, rows + 2 * reach, ny), f32),
            pltpu.VMEM(tile, f32), pltpu.VMEM(tile, f32), pltpu.VMEM(tile, f32), pltpu.VMEM(tile, f32), pltpu.VMEM(tile, f32),
            dma((4,)), dma((4,)), dma((2,)), dma((4,)), dma((4,)), dma((4,)), dma((2,)), dma((2,)),
        ],
        compiler_params=pltpu.CompilerParams(has_side_effects=True, collective_id=0, vmem_limit_bytes=limit), name="flow",
    )(flow_state, jnp.asarray(band_matrix()), owner)
    sent = pl.pallas_call(
        functools.partial(compact_kernel, n_tile),
        out_shape=shape((n_tile, rows, cap + 2 * LANES), f32),
        in_specs=[smem, smem, vmem, vmem], out_specs=vmem,
        scratch_shapes=[pltpu.VMEM((n_tile, rows, LANES), f32)],
        compiler_params=pltpu.CompilerParams(vmem_limit_bytes=limit), name="compact",
    )(base, count, coeffs, place)
    chunks = 4 if cap % (4 * LANES) == 0 else 1
    record = pl.pallas_call(
        functools.partial(record_kernel, n_tile, chunks),
        out_shape=shape((nx, cap), f32),
        in_specs=[vmem, vmem], out_specs=vmem,
        scratch_shapes=[
            pltpu.VMEM((n_tile, rows, cap), f32), pltpu.VMEM((3, nx, cap), f32),
            dma((n_tile, chunks)), dma((n_tile, chunks)), dma((chunks,)), dma((3, chunks)),
        ],
        compiler_params=pltpu.CompilerParams(has_side_effects=True, collective_id=1, vmem_limit_bytes=limit), name="record",
    )(sent, jnp.asarray(lift_matrix(nx).astype(np.float32)))
    return record[None, None]


def solution(mesh):
    in_specs = (P("grp", None, "tile", None), P())
    out_specs = P("grp", "tile", None, None)
    run = functools.partial(body, n_tile=mesh.shape["tile"])
    return jax.shard_map(run, mesh=mesh, in_specs=in_specs, out_specs=out_specs, check_vma=False)
```

```python
import functools

import jax
import jax.numpy as jnp
import numpy as np
from jax import lax
from jax.experimental import pallas as pl
from jax.experimental.pallas import tpu as pltpu
from jax.sharding import PartitionSpec as P

time_step = 0.2
viscosity = 0.05
reach = 4
first_coeffs = (0.8, -0.2, 4.0 / 105.0, -1.0 / 280.0)
second_center = -205.0 / 72.0
second_coeffs = (1.6, -0.2, 8.0 / 315.0, -1.0 / 560.0)
lift_alpha = -1.586134342059924
lift_beta = -0.052980118572961
lift_gamma = 0.882911075530934
lift_delta = 0.443506852043971
lift_scale = 1.149604398860241
LANES = 128
MESH = pl.DeviceIdType.MESH


def lift_numpy(signal):
    even, odd = signal[0::2].copy(), signal[1::2].copy()
    odd += lift_alpha * (even + np.roll(even, -1, 0))
    even += lift_beta * (odd + np.roll(odd, 1, 0))
    odd += lift_gamma * (even + np.roll(even, -1, 0))
    even += lift_delta * (odd + np.roll(odd, 1, 0))
    return np.concatenate([even * lift_scale, odd / lift_scale])


def lift_matrix(length):
    return lift_numpy(np.eye(length))


def band_matrix():
    full = lift_matrix(8 * LANES)
    low = full[LANES : 2 * LANES, LANES : 5 * LANES]
    high = full[4 * LANES + LANES : 4 * LANES + 2 * LANES, LANES : 5 * LANES]
    return np.concatenate([low, high]).T.astype(np.float32)


def shifted_y(value, k):
    return pltpu.roll(value, (-k) % value.shape[-1], value.ndim - 1)


def derivatives(center, shift, want_first=True, want_second=True):
    first, second = None, second_center * center if want_second else None
    for k in range(1, reach + 1):
        ahead, behind = shift(k), shift(-k)
        if want_first:
            term = first_coeffs[k - 1] * (ahead - behind)
            first = term if first is None else first + term
        if want_second:
            second = second + second_coeffs[k - 1] * (ahead + behind)
    return first, second


def slots_of(n_tile, owner_ref, place_ref, base_ref, count_ref):
    owner = owner_ref[...]
    n_blocks = owner.shape[0]
    upper = (lax.broadcasted_iota(jnp.int32, (LANES, LANES), 0) <= lax.broadcasted_iota(jnp.int32, (LANES, LANES), 1)).astype(jnp.float32)
    lower = (lax.broadcasted_iota(jnp.int32, (n_blocks, n_blocks), 0) > lax.broadcasted_iota(jnp.int32, (n_blocks, n_blocks), 1)).astype(jnp.float32)
    lane = lax.broadcasted_iota(jnp.int32, (n_blocks, LANES), 1)

    def step(s, carry):
        place, counts, ahead = carry
        mask = (owner == s).astype(jnp.float32)
        within = jnp.dot(mask, upper, preferred_element_type=jnp.float32)
        total = jnp.sum(mask, axis=1, keepdims=True)
        place = place + mask * (ahead + within - 1.0)
        counts = jnp.where(lane == s, total, counts)
        return place, counts, ahead + total

    zeros = jnp.zeros((n_blocks, LANES), jnp.float32)
    carry = (zeros, zeros, jnp.zeros((n_blocks, 1), jnp.float32))
    if n_tile <= 16:
        for s in range(n_tile):
            carry = step(s, carry)
    else:
        carry = lax.fori_loop(0, n_tile, step, carry)
    place, counts, _ = carry
    place_ref[...] = place
    count_ref[...] = counts.astype(jnp.int32)
    base_ref[...] = jnp.dot(lower, counts, preferred_element_type=jnp.float32).astype(jnp.int32)


def flow_kernel(n_tile, own_ref, band_ref, owner_ref, out_ref, place_ref, base_ref, count_ref,
                fields, mids, halo, mid_halo, pad, ppad, middle, fin, along_y, along_z, lap, send_sem, recv_sem, hsend_sem, hrecv_sem, msend_sem, mrecv_sem, mhsend_sem, mhrecv_sem, relay_sem):
    g, t = lax.axis_index("grp"), lax.axis_index("tile")
    right, left = lax.rem(t + 1, n_tile), lax.rem(t + n_tile - 1, n_tile)
    planes, rows, ny = own_ref.shape[1:]
    own = own_ref.at[0]

    barrier = pltpu.get_barrier_semaphore()
    for k in range(1, 4):
        pl.semaphore_signal(barrier, inc=1, device_id=(lax.rem(g + k, 4), t), device_id_type=MESH)
    for side in (right, left):
        pl.semaphore_signal(barrier, inc=1, device_id=(g, side), device_id_type=MESH)

    @pl.when((g == 0) | (g == 3))
    def _():
        for side in (right, left):
            pl.semaphore_signal(barrier, inc=1, device_id=(3 - g, side), device_id_type=MESH)
        pl.semaphore_wait(barrier, 7)

    @pl.when((g == 1) | (g == 2))
    def _():
        pl.semaphore_wait(barrier, 5)

    def gather_copy(src, dst, ssem, rsem, k, slot):
        return pltpu.make_async_remote_copy(
            src_ref=src, dst_ref=dst.at[slot], send_sem=ssem.at[k], recv_sem=rsem.at[slot],
            device_id=(k, t), device_id_type=MESH)

    half = planes // 2

    def whole_copy(k, slot):
        return pltpu.make_async_remote_copy(
            src_ref=own, dst_ref=fields.at[slot], send_sem=send_sem.at[k], recv_sem=recv_sem.at[slot, 0],
            device_id=(k, t), device_id_type=MESH)

    def half_copy(slot, k):
        part = pl.ds(k * half, half)
        return pltpu.make_async_remote_copy(
            src_ref=own.at[part], dst_ref=fields.at[slot, part], send_sem=send_sem.at[k],
            recv_sem=recv_sem.at[slot, k], device_id=(k, t), device_id_type=MESH)

    def relay_copy(slot, k):
        part = pl.ds(k * half, half)
        return pltpu.make_async_remote_copy(
            src_ref=fields.at[slot, part], dst_ref=fields.at[slot, part], send_sem=relay_sem.at[slot],
            recv_sem=recv_sem.at[slot, k], device_id=(1 - k, t), device_id_type=MESH)

    def halo_copy(src, dst, ssem, rsem, side, slot, group):
        return pltpu.make_async_remote_copy(
            src_ref=src, dst_ref=dst.at[slot + side], send_sem=ssem.at[side], recv_sem=rsem.at[slot + side],
            device_id=(group, right if side == 0 else left), device_id_type=MESH)

    @pl.when(g < 3)
    def _():
        for side in range(2):
            halo_copy(own, halo, hsend_sem, hrecv_sem, side, 0, g).start()

    for k in range(3):
        @pl.when((g < 2) & (g != k))
        def _(k=k):
            whole_copy(k, g).start()

    @pl.when(g >= 2)
    def _():
        for k in range(2):
            half_copy(g, k).start()

    @pl.when(g == 3)
    def _():
        whole_copy(2, 3).start()
        for side in range(2):
            halo_copy(own, halo, hsend_sem, hrecv_sem, side, 2, 0).start()

    def local_terms():
        for z in range(planes):
            center = pad[z, reach : reach + rows]
            fy, sy = derivatives(center, lambda k: shifted_y(center, k))
            fz, sz = derivatives(center, lambda k: pad[(z + k) % planes, reach : reach + rows])
            along_y[z], along_z[z], lap[z] = fy, fz, sy + sz

    slots_of(n_tile, owner_ref, place_ref, base_ref, count_ref)

    @pl.when(g < 3)
    def _():
        for k in range(3):
            @pl.when(g == k)
            def _(k=k):
                fields[k] = own_ref[0]

        for z in range(planes):
            pad[z, reach : reach + rows] = own_ref[0, z]
        local_terms()

        @pl.when(g < 2)
        def _():
            for slot in (2, 3):
                half_copy(slot, g).wait_recv()
                relay_copy(slot, g).start()
            whole_copy(0, 1 - g).wait_recv()
            for slot in (2, 3):
                half_copy(slot, 1 - g).wait_recv()

        @pl.when(g == 2)
        def _():
            for slot in (0, 1, 3):
                whole_copy(0, slot).wait_recv()

        for side in range(2):
            halo_copy(own, halo, hsend_sem, hrecv_sem, side, 0, g).wait_recv()

        @pl.when(g == 0)
        def _():
            for side in range(2):
                halo_copy(own, halo, hsend_sem, hrecv_sem, side, 2, 0).wait_recv()
            for z in range(planes):
                ppad[z, 0:reach] = halo[2, z, rows - reach : rows]
                ppad[z, reach : reach + rows] = fields[3, z]
                ppad[z, reach + rows : 2 * reach + rows] = halo[3, z, 0:reach]
            for z in range(planes):
                middle[z], _ = derivatives(None, lambda k: ppad[z, reach + k : reach + k + rows], True, False)

        @pl.when(g == 1)
        def _():
            for z in range(planes):
                value = fields[3, z]
                middle[z], _ = derivatives(None, lambda k: shifted_y(value, k), True, False)

        @pl.when(g == 2)
        def _():
            for z in range(planes):
                middle[z], _ = derivatives(None, lambda k: fields[3, (z + k) % planes], True, False)

        def tendency(z, vel, press):
            center = pad[z, reach : reach + rows]
            fx, sx = derivatives(center, lambda k: pad[z, reach + k : reach + k + rows])
            advect = vel[0, z] * fx + vel[1, z] * along_y[z] + vel[2, z] * along_z[z]
            return viscosity * (sx + lap[z]) - advect - press

        for z in range(planes):
            pad[z, 0:reach] = halo[0, z, rows - reach : rows]
            pad[z, reach + rows : 2 * reach + rows] = halo[1, z, 0:reach]
        for z in range(planes):
            press = middle[z]
            ppad[z, 0:rows] = press
        for z in range(planes):
            middle[z] = own_ref[0, z] + time_step * tendency(z, fields, ppad[z, 0:rows])

        for side in range(2):
            halo_copy(middle, mid_halo, mhsend_sem, mhrecv_sem, side, 0, g).start()
        for k in range(3):
            @pl.when(g != k)
            def _(k=k):
                gather_copy(middle, mids, msend_sem, mrecv_sem, k, g).start()

            @pl.when(g == k)
            def _(k=k):
                mids[k] = middle[...]

        for z in range(planes):
            pad[z, reach : reach + rows] = middle[z]
        local_terms()
        for k in range(3):
            @pl.when(g != k)
            def _(k=k):
                gather_copy(middle, mids, msend_sem, mrecv_sem, 0, k).wait_recv()
        for side in range(2):
            halo_copy(middle, mid_halo, mhsend_sem, mhrecv_sem, side, 0, g).wait_recv()
        for z in range(planes):
            pad[z, 0:reach] = mid_halo[0, z, rows - reach : rows]
            pad[z, reach + rows : 2 * reach + rows] = mid_halo[1, z, 0:reach]
        for z in range(planes):
            fin[z] = 0.5 * ((own_ref[0, z] + middle[z]) + time_step * tendency(z, mids, ppad[z, 0:rows]))

        blocks = ny // (2 * LANES)
        groups = ny // LANES
        for z in range(planes):
            value = fin[z]
            pieces = []
            for b in range(blocks):
                window = [value[:, ((2 * b + j) % groups) * LANES : ((2 * b + j) % groups + 1) * LANES] for j in (-1, 0, 1, 2)]
                pieces.append(jnp.concatenate(window, axis=1))
            stacked = jnp.concatenate(pieces, axis=0)
            lifted = jnp.dot(stacked, band_ref[...], precision=lax.Precision.HIGHEST, preferred_element_type=jnp.float32)
            for b in range(blocks):
                piece = lifted[b * rows : (b + 1) * rows]
                fin[z, :, b * LANES : (b + 1) * LANES] = piece[:, 0:LANES]
                fin[z, :, ny // 2 + b * LANES : ny // 2 + (b + 1) * LANES] = piece[:, LANES:]

        even = [fin[2 * i] for i in range(half)]
        odd = [fin[2 * i + 1] for i in range(half)]
        odd = [odd[i] + lift_alpha * (even[i] + even[(i + 1) % half]) for i in range(half)]
        even = [even[i] + lift_beta * (odd[i] + odd[(i - 1) % half]) for i in range(half)]
        odd = [odd[i] + lift_gamma * (even[i] + even[(i + 1) % half]) for i in range(half)]
        even = [even[i] + lift_delta * (odd[i] + odd[(i - 1) % half]) for i in range(half)]
        for i in range(half):
            out_ref[i] = even[i] * lift_scale
            out_ref[half + i] = odd[i] * (1.0 / lift_scale)

        for side in range(2):
            halo_copy(middle, mid_halo, mhsend_sem, mhrecv_sem, side, 0, g).wait_send()
        for k in range(3):
            @pl.when(g != k)
            def _(k=k):
                gather_copy(middle, mids, msend_sem, mrecv_sem, k, g).wait_send()

    @pl.when(g == 3)
    def _():
        out_ref[...] = jnp.zeros_like(out_ref)

    for side in range(2):
        halo_copy(own, halo, hsend_sem, hrecv_sem, side, 0, g).wait_send()
    for k in range(3):
        @pl.when((g < 2) & (g != k))
        def _(k=k):
            whole_copy(k, g).wait_send()

    @pl.when(g < 2)
    def _():
        for slot in (2, 3):
            relay_copy(slot, g).wait_send()

    @pl.when(g >= 2)
    def _():
        for k in range(2):
            half_copy(g, k).wait_send()

    @pl.when(g == 3)
    def _():
        whole_copy(2, 3).wait_send()


def compact_kernel(n_tile, base_ref, count_ref, coeff_ref, place_ref, out_ref, current):
    planes, rows, ny = coeff_ref.shape
    groups = ny // LANES
    out_ref[...] = jnp.zeros_like(out_ref)
    current[...] = jnp.zeros_like(current)
    rank = lax.broadcasted_iota(jnp.int32, (LANES, LANES), 0).astype(jnp.float32)
    lane = lax.broadcasted_iota(jnp.int32, (rows, LANES), 1)

    def sort(b):
        z, y = b // groups, b % groups
        value = coeff_ref[z, :, pl.ds(pl.multiple_of(y * LANES, LANES), LANES)]
        high = value.astype(jnp.bfloat16).astype(jnp.float32)
        rest = value - high
        mid = rest.astype(jnp.bfloat16).astype(jnp.float32)
        low = rest - mid
        parts = jnp.concatenate([high, mid, low], axis=0).astype(jnp.bfloat16)
        chosen = jnp.where(rank == place_ref[pl.ds(b, 1), :], 1.0, 0.0).astype(jnp.bfloat16)
        ordered = lax.dot_general(parts, chosen, (((1,), (1,)), ((), ())), preferred_element_type=jnp.float32)
        return (ordered[0:rows] + ordered[rows : 2 * rows]) + ordered[2 * rows : 3 * rows]

    def pencil(b, ordered, s, ahead):
        base, count = base_ref[b, s], count_ref[b, s]
        start = base & (LANES - 1)
        end = start + count
        turned = pltpu.roll(ordered, (start - ahead) & (LANES - 1), 1)
        now = current[s] + jnp.where((lane >= start) & (lane < end), turned, 0.0)
        group = pl.multiple_of(base - start, LANES)
        after = jnp.where(lane < end - LANES, turned, 0.0)
        current[s] = jnp.where(end >= LANES, after, now)
        out_ref[s, :, pl.ds(group, 2 * LANES)] = jnp.concatenate([now, after], axis=1)
        return ahead + count

    n_blocks = planes * groups
    batch = 8 if n_blocks % 8 == 0 and n_tile <= 16 else 1

    def blocks(i, _):
        ordered = [sort(i * batch + j) for j in range(batch)]
        for j in range(batch):
            b = i * batch + j
            if n_tile <= 16:
                ahead = jnp.int32(0)
                for s in range(n_tile):
                    ahead = pencil(b, ordered[j], s, ahead)
            else:
                lax.fori_loop(0, n_tile, lambda s, ahead: pencil(b, ordered[j], s, ahead), jnp.int32(0))
        return 0

    lax.fori_loop(0, n_blocks // batch, blocks, 0)


def record_kernel(n_tile, chunks, sent_ref, matrix_ref, out_ref, got, records, send_sem, recv_sem, rsend_sem, rrecv_sem):
    g, t = lax.axis_index("grp"), lax.axis_index("tile")
    rows, nx, cap = sent_ref.shape[1], out_ref.shape[0], out_ref.shape[1]
    width = cap // chunks

    barrier = pltpu.get_barrier_semaphore()

    @pl.when(g < 3)
    def _():
        for k in range(1, n_tile):
            pl.semaphore_signal(barrier, inc=1, device_id=(g, lax.rem(t + k, n_tile)), device_id_type=MESH)
        pl.semaphore_signal(barrier, inc=1, device_id=(3, t), device_id_type=MESH)
        pl.semaphore_wait(barrier, n_tile)

    @pl.when(g == 3)
    def _():
        for k in range(3):
            pl.semaphore_signal(barrier, inc=1, device_id=(k, t), device_id_type=MESH)
        pl.semaphore_wait(barrier, 3)

    def exchange(s, slot, c):
        part = pl.ds(c * width, width)
        return pltpu.make_async_remote_copy(
            src_ref=sent_ref.at[s, :, part], dst_ref=got.at[slot, :, part], send_sem=send_sem.at[s, c],
            recv_sem=recv_sem.at[slot, c], device_id=(g, s), device_id_type=MESH)

    def report(c, slot):
        part = pl.ds(c * width, width)
        return pltpu.make_async_remote_copy(
            src_ref=out_ref.at[:, part], dst_ref=records.at[slot, :, part], send_sem=rsend_sem.at[c],
            recv_sem=rrecv_sem.at[slot, c], device_id=(3, t), device_id_type=MESH)

    @pl.when(g < 3)
    def _():
        for c in range(chunks):
            for k in range(1, n_tile):
                exchange(lax.rem(t + k, n_tile), t, c).start()
        got[t] = sent_ref[t, :, 0:cap]
        matrix = matrix_ref[...]
        for c in range(chunks):
            for k in range(1, n_tile):
                exchange(lax.rem(t + k, n_tile), lax.rem(t + k, n_tile), c).wait_recv()
            value = got[:, :, c * width : (c + 1) * width].reshape(nx, width)
            out_ref[:, c * width : (c + 1) * width] = jnp.dot(
                matrix, value, precision=lax.Precision.HIGHEST, preferred_element_type=jnp.float32)
            report(c, g).start()
        for c in range(chunks):
            for k in range(1, n_tile):
                exchange(lax.rem(t + k, n_tile), t, c).wait_send()
            report(c, g).wait_send()

    @pl.when(g == 3)
    def _():
        for c in range(chunks):
            for k in range(3):
                report(c, k).wait_recv()
            part = slice(c * width, (c + 1) * width)
            first, second, third = records[0, :, part], records[1, :, part], records[2, :, part]
            out_ref[:, part] = first * first + second * second + third * third


def body(flow_state, line_owner, *, n_tile):
    _, planes, rows, ny = flow_state.shape
    n_lines = line_owner.shape[0]
    n_blocks = n_lines // LANES
    nx = rows * n_tile
    cap = 2 * planes * ny // n_tile
    vmem = pl.BlockSpec(memory_space=pltpu.VMEM)
    smem = pl.BlockSpec(memory_space=pltpu.SMEM)
    f32 = jnp.float32
    shape = jax.ShapeDtypeStruct
    limit = 16 * 1024 * 1024
    dma = pltpu.SemaphoreType.DMA
    owner = line_owner.reshape(n_blocks, LANES)
    tile = (planes, rows, ny)
    ints = shape((n_blocks, LANES), jnp.int32)
    coeffs, place, base, count = pl.pallas_call(
        functools.partial(flow_kernel, n_tile),
        out_shape=(shape(tile, f32), shape((n_blocks, LANES), f32), ints, ints),
        in_specs=[vmem, vmem, vmem], out_specs=(vmem, vmem, vmem, vmem),
        scratch_shapes=[
            pltpu.VMEM((4,) + tile, f32), pltpu.VMEM((3,) + tile, f32),
            pltpu.VMEM((4,) + tile, f32), pltpu.VMEM((2,) + tile, f32),
            pltpu.VMEM((planes, rows + 2 * reach, ny), f32), pltpu.VMEM((planes, rows + 2 * reach, ny), f32),
            pltpu.VMEM(tile, f32), pltpu.VMEM(tile, f32), pltpu.VMEM(tile, f32), pltpu.VMEM(tile, f32), pltpu.VMEM(tile, f32),
            dma((4,)), dma((4, 2)), dma((2,)), dma((4,)), dma((4,)), dma((4,)), dma((2,)), dma((2,)), dma((4,)),
        ],
        compiler_params=pltpu.CompilerParams(has_side_effects=True, collective_id=0, vmem_limit_bytes=limit), name="flow",
    )(flow_state, jnp.asarray(band_matrix()), owner)
    sent = pl.pallas_call(
        functools.partial(compact_kernel, n_tile),
        out_shape=shape((n_tile, rows, cap + 2 * LANES), f32),
        in_specs=[smem, smem, vmem, vmem], out_specs=vmem,
        scratch_shapes=[pltpu.VMEM((n_tile, rows, LANES), f32)],
        compiler_params=pltpu.CompilerParams(vmem_limit_bytes=limit), name="compact",
    )(base, count, coeffs, place)
    chunks = 4 if cap % (4 * LANES) == 0 else 1
    record = pl.pallas_call(
        functools.partial(record_kernel, n_tile, chunks),
        out_shape=shape((nx, cap), f32),
        in_specs=[vmem, vmem], out_specs=vmem,
        scratch_shapes=[
            pltpu.VMEM((n_tile, rows, cap), f32), pltpu.VMEM((3, nx, cap), f32),
            dma((n_tile, chunks)), dma((n_tile, chunks)), dma((chunks,)), dma((3, chunks)),
        ],
        compiler_params=pltpu.CompilerParams(has_side_effects=True, collective_id=1, vmem_limit_bytes=limit), name="record",
    )(sent, jnp.asarray(lift_matrix(nx).astype(np.float32)))
    return record[None, None]


def solution(mesh):
    in_specs = (P("grp", None, "tile", None), P())
    out_specs = P("grp", "tile", None, None)
    run = functools.partial(body, n_tile=mesh.shape["tile"])
    return jax.shard_map(run, mesh=mesh, in_specs=in_specs, out_specs=out_specs, check_vma=False)
```

```python
import functools

import jax
import jax.numpy as jnp
import numpy as np
from jax import lax
from jax.experimental import pallas as pl
from jax.experimental.pallas import tpu as pltpu
from jax.sharding import PartitionSpec as P

time_step = 0.2
viscosity = 0.05
reach = 4
first_coeffs = (0.8, -0.2, 4.0 / 105.0, -1.0 / 280.0)
second_center = -205.0 / 72.0
second_coeffs = (1.6, -0.2, 8.0 / 315.0, -1.0 / 560.0)
lift_alpha = -1.586134342059924
lift_beta = -0.052980118572961
lift_gamma = 0.882911075530934
lift_delta = 0.443506852043971
lift_scale = 1.149604398860241
LANES = 128
MESH = pl.DeviceIdType.MESH


def lift_numpy(signal):
    even, odd = signal[0::2].copy(), signal[1::2].copy()
    odd += lift_alpha * (even + np.roll(even, -1, 0))
    even += lift_beta * (odd + np.roll(odd, 1, 0))
    odd += lift_gamma * (even + np.roll(even, -1, 0))
    even += lift_delta * (odd + np.roll(odd, 1, 0))
    return np.concatenate([even * lift_scale, odd / lift_scale])


def lift_matrix(length):
    return lift_numpy(np.eye(length))


def band_matrix():
    full = lift_matrix(8 * LANES)
    low = full[LANES : 2 * LANES, LANES : 5 * LANES]
    high = full[4 * LANES + LANES : 4 * LANES + 2 * LANES, LANES : 5 * LANES]
    return np.concatenate([low, high]).T.astype(np.float32)


def band_value(taps_low, taps_high):
    row = lax.broadcasted_iota(jnp.int32, (4 * LANES, 2 * LANES), 0)
    column = lax.broadcasted_iota(jnp.int32, (4 * LANES, 2 * LANES), 1)
    distance = row - LANES - 2 * (column & (LANES - 1))
    is_low = column < LANES
    value = jnp.zeros((4 * LANES, 2 * LANES), jnp.float32)
    for offset in range(-4, 5):
        tap = jnp.where(is_low, taps_low[offset + 4], taps_high[offset + 4])
        value = jnp.where(distance == offset, tap, value)
    return value


def band_taps():
    band = band_matrix()
    rows = slice(LANES + LANES // 2 - 4, LANES + LANES // 2 + 5)
    return [float(x) for x in band[rows, LANES // 4]], [float(x) for x in band[rows, LANES + LANES // 4]]


def shifted_y(value, k):
    return pltpu.roll(value, (-k) % value.shape[-1], value.ndim - 1)


def derivatives(center, shift, want_first=True, want_second=True):
    first, second = None, second_center * center if want_second else None
    for k in range(1, reach + 1):
        ahead, behind = shift(k), shift(-k)
        if want_first:
            term = first_coeffs[k - 1] * (ahead - behind)
            first = term if first is None else first + term
        if want_second:
            second = second + second_coeffs[k - 1] * (ahead + behind)
    return first, second


def slots_of(n_tile, owner_ref, place_ref, base_ref, count_ref):
    owner = owner_ref[...]
    n_blocks = owner.shape[0]
    upper = (lax.broadcasted_iota(jnp.int32, (LANES, LANES), 0) <= lax.broadcasted_iota(jnp.int32, (LANES, LANES), 1)).astype(jnp.float32)
    lower = (lax.broadcasted_iota(jnp.int32, (n_blocks, n_blocks), 0) > lax.broadcasted_iota(jnp.int32, (n_blocks, n_blocks), 1)).astype(jnp.float32)
    lane = lax.broadcasted_iota(jnp.int32, (n_blocks, LANES), 1)

    def step(s, carry):
        place, counts, ahead = carry
        mask = (owner == s).astype(jnp.float32)
        within = jnp.dot(mask, upper, preferred_element_type=jnp.float32)
        total = jnp.sum(mask, axis=1, keepdims=True)
        place = place + mask * (ahead + within - 1.0)
        counts = jnp.where(lane == s, total, counts)
        return place, counts, ahead + total

    zeros = jnp.zeros((n_blocks, LANES), jnp.float32)
    carry = (zeros, zeros, jnp.zeros((n_blocks, 1), jnp.float32))
    if n_tile <= 16:
        for s in range(n_tile):
            carry = step(s, carry)
    else:
        carry = lax.fori_loop(0, n_tile, step, carry)
    place, counts, _ = carry
    place_ref[...] = place
    count_ref[...] = counts.astype(jnp.int32)
    base_ref[...] = jnp.dot(lower, counts, preferred_element_type=jnp.float32).astype(jnp.int32)


def flow_kernel(n_tile, own_ref, owner_ref, out_ref, place_ref, base_ref, count_ref,
                fields, mids, halo, mid_halo, pad, ppad, middle, fin, along_y, along_z, lap, send_sem, recv_sem, hsend_sem, hrecv_sem, msend_sem, mrecv_sem, mhsend_sem, mhrecv_sem, relay_sem, band_ref):
    g, t = lax.axis_index("grp"), lax.axis_index("tile")
    right, left = lax.rem(t + 1, n_tile), lax.rem(t + n_tile - 1, n_tile)
    planes, rows, ny = own_ref.shape[1:]
    own = own_ref.at[0]

    barrier = pltpu.get_barrier_semaphore()
    for k in range(1, 4):
        pl.semaphore_signal(barrier, inc=1, device_id=(lax.rem(g + k, 4), t), device_id_type=MESH)
    for side in (right, left):
        pl.semaphore_signal(barrier, inc=1, device_id=(g, side), device_id_type=MESH)

    @pl.when((g == 0) | (g == 3))
    def _():
        for side in (right, left):
            pl.semaphore_signal(barrier, inc=1, device_id=(3 - g, side), device_id_type=MESH)
        pl.semaphore_wait(barrier, 7)

    @pl.when((g == 1) | (g == 2))
    def _():
        pl.semaphore_wait(barrier, 5)

    def gather_copy(src, dst, ssem, rsem, k, slot):
        return pltpu.make_async_remote_copy(
            src_ref=src, dst_ref=dst.at[slot], send_sem=ssem.at[k], recv_sem=rsem.at[slot],
            device_id=(k, t), device_id_type=MESH)

    half = planes // 2

    def whole_copy(k, slot):
        return pltpu.make_async_remote_copy(
            src_ref=own, dst_ref=fields.at[slot], send_sem=send_sem.at[k], recv_sem=recv_sem.at[slot, 0],
            device_id=(k, t), device_id_type=MESH)

    def half_copy(slot, k):
        part = pl.ds(k * half, half)
        return pltpu.make_async_remote_copy(
            src_ref=own.at[part], dst_ref=fields.at[slot, part], send_sem=send_sem.at[k],
            recv_sem=recv_sem.at[slot, k], device_id=(k, t), device_id_type=MESH)

    def relay_copy(slot, k):
        part = pl.ds(k * half, half)
        return pltpu.make_async_remote_copy(
            src_ref=fields.at[slot, part], dst_ref=fields.at[slot, part], send_sem=relay_sem.at[slot],
            recv_sem=recv_sem.at[slot, k], device_id=(1 - k, t), device_id_type=MESH)

    def halo_copy(src, dst, ssem, rsem, side, slot, group):
        return pltpu.make_async_remote_copy(
            src_ref=src, dst_ref=dst.at[slot + side], send_sem=ssem.at[side], recv_sem=rsem.at[slot + side],
            device_id=(group, right if side == 0 else left), device_id_type=MESH)

    @pl.when(g < 3)
    def _():
        for side in range(2):
            halo_copy(own, halo, hsend_sem, hrecv_sem, side, 0, g).start()

    for k in range(3):
        @pl.when((g < 2) & (g != k))
        def _(k=k):
            whole_copy(k, g).start()

    @pl.when(g >= 2)
    def _():
        for k in range(2):
            half_copy(g, k).start()

    @pl.when(g == 3)
    def _():
        whole_copy(2, 3).start()
        for side in range(2):
            halo_copy(own, halo, hsend_sem, hrecv_sem, side, 2, 0).start()

    def local_terms():
        for z in range(planes):
            center = pad[z, reach : reach + rows]
            fy, sy = derivatives(center, lambda k: shifted_y(center, k))
            fz, sz = derivatives(center, lambda k: pad[(z + k) % planes, reach : reach + rows])
            along_y[z], along_z[z], lap[z] = fy, fz, sy + sz

    slots_of(n_tile, owner_ref, place_ref, base_ref, count_ref)
    band_ref[...] = band_value(*band_taps())

    @pl.when(g < 3)
    def _():
        for k in range(3):
            @pl.when(g == k)
            def _(k=k):
                fields[k] = own_ref[0]

        for z in range(planes):
            pad[z, reach : reach + rows] = own_ref[0, z]
        local_terms()

        @pl.when(g < 2)
        def _():
            for slot in (2, 3):
                half_copy(slot, g).wait_recv()
                relay_copy(slot, g).start()
            whole_copy(0, 1 - g).wait_recv()
            for slot in (2, 3):
                half_copy(slot, 1 - g).wait_recv()

        @pl.when(g == 2)
        def _():
            for slot in (0, 1, 3):
                whole_copy(0, slot).wait_recv()

        for side in range(2):
            halo_copy(own, halo, hsend_sem, hrecv_sem, side, 0, g).wait_recv()

        @pl.when(g == 0)
        def _():
            for side in range(2):
                halo_copy(own, halo, hsend_sem, hrecv_sem, side, 2, 0).wait_recv()
            for z in range(planes):
                ppad[z, 0:reach] = halo[2, z, rows - reach : rows]
                ppad[z, reach : reach + rows] = fields[3, z]
                ppad[z, reach + rows : 2 * reach + rows] = halo[3, z, 0:reach]
            for z in range(planes):
                middle[z], _ = derivatives(None, lambda k: ppad[z, reach + k : reach + k + rows], True, False)

        @pl.when(g == 1)
        def _():
            for z in range(planes):
                value = fields[3, z]
                middle[z], _ = derivatives(None, lambda k: shifted_y(value, k), True, False)

        @pl.when(g == 2)
        def _():
            for z in range(planes):
                middle[z], _ = derivatives(None, lambda k: fields[3, (z + k) % planes], True, False)

        def tendency(z, vel, press):
            center = pad[z, reach : reach + rows]
            fx, sx = derivatives(center, lambda k: pad[z, reach + k : reach + k + rows])
            advect = vel[0, z] * fx + vel[1, z] * along_y[z] + vel[2, z] * along_z[z]
            return viscosity * (sx + lap[z]) - advect - press

        for z in range(planes):
            pad[z, 0:reach] = halo[0, z, rows - reach : rows]
            pad[z, reach + rows : 2 * reach + rows] = halo[1, z, 0:reach]
        for z in range(planes):
            press = middle[z]
            ppad[z, 0:rows] = press
        for z in range(planes):
            middle[z] = own_ref[0, z] + time_step * tendency(z, fields, ppad[z, 0:rows])

        for side in range(2):
            halo_copy(middle, mid_halo, mhsend_sem, mhrecv_sem, side, 0, g).start()
        for k in range(3):
            @pl.when(g != k)
            def _(k=k):
                gather_copy(middle, mids, msend_sem, mrecv_sem, k, g).start()

            @pl.when(g == k)
            def _(k=k):
                mids[k] = middle[...]

        for z in range(planes):
            pad[z, reach : reach + rows] = middle[z]
        local_terms()
        for k in range(3):
            @pl.when(g != k)
            def _(k=k):
                gather_copy(middle, mids, msend_sem, mrecv_sem, 0, k).wait_recv()
        for side in range(2):
            halo_copy(middle, mid_halo, mhsend_sem, mhrecv_sem, side, 0, g).wait_recv()
        for z in range(planes):
            pad[z, 0:reach] = mid_halo[0, z, rows - reach : rows]
            pad[z, reach + rows : 2 * reach + rows] = mid_halo[1, z, 0:reach]
        for z in range(planes):
            fin[z] = 0.5 * ((own_ref[0, z] + middle[z]) + time_step * tendency(z, mids, ppad[z, 0:rows]))

        blocks = ny // (2 * LANES)
        groups = ny // LANES
        for z in range(planes):
            value = fin[z]
            pieces = []
            for b in range(blocks):
                window = [value[:, ((2 * b + j) % groups) * LANES : ((2 * b + j) % groups + 1) * LANES] for j in (-1, 0, 1, 2)]
                pieces.append(jnp.concatenate(window, axis=1))
            stacked = jnp.concatenate(pieces, axis=0)
            lifted = jnp.dot(stacked, band_ref[...], precision=lax.Precision.HIGHEST, preferred_element_type=jnp.float32)
            for b in range(blocks):
                piece = lifted[b * rows : (b + 1) * rows]
                fin[z, :, b * LANES : (b + 1) * LANES] = piece[:, 0:LANES]
                fin[z, :, ny // 2 + b * LANES : ny // 2 + (b + 1) * LANES] = piece[:, LANES:]

        even = [fin[2 * i] for i in range(half)]
        odd = [fin[2 * i + 1] for i in range(half)]
        odd = [odd[i] + lift_alpha * (even[i] + even[(i + 1) % half]) for i in range(half)]
        even = [even[i] + lift_beta * (odd[i] + odd[(i - 1) % half]) for i in range(half)]
        odd = [odd[i] + lift_gamma * (even[i] + even[(i + 1) % half]) for i in range(half)]
        even = [even[i] + lift_delta * (odd[i] + odd[(i - 1) % half]) for i in range(half)]
        for i in range(half):
            out_ref[i] = even[i] * lift_scale
            out_ref[half + i] = odd[i] * (1.0 / lift_scale)

        for side in range(2):
            halo_copy(middle, mid_halo, mhsend_sem, mhrecv_sem, side, 0, g).wait_send()
        for k in range(3):
            @pl.when(g != k)
            def _(k=k):
                gather_copy(middle, mids, msend_sem, mrecv_sem, k, g).wait_send()

    @pl.when(g == 3)
    def _():
        out_ref[...] = jnp.zeros_like(out_ref)

    for side in range(2):
        halo_copy(own, halo, hsend_sem, hrecv_sem, side, 0, g).wait_send()
    for k in range(3):
        @pl.when((g < 2) & (g != k))
        def _(k=k):
            whole_copy(k, g).wait_send()

    @pl.when(g < 2)
    def _():
        for slot in (2, 3):
            relay_copy(slot, g).wait_send()

    @pl.when(g >= 2)
    def _():
        for k in range(2):
            half_copy(g, k).wait_send()

    @pl.when(g == 3)
    def _():
        whole_copy(2, 3).wait_send()


def compact_kernel(n_tile, base_ref, count_ref, coeff_ref, place_ref, out_ref, current):
    planes, rows, ny = coeff_ref.shape
    groups = ny // LANES
    out_ref[...] = jnp.zeros_like(out_ref)
    current[...] = jnp.zeros_like(current)
    rank = lax.broadcasted_iota(jnp.int32, (LANES, LANES), 0).astype(jnp.float32)
    lane = lax.broadcasted_iota(jnp.int32, (rows, LANES), 1)

    def sort(b):
        z, y = b // groups, b % groups
        value = coeff_ref[z, :, pl.ds(pl.multiple_of(y * LANES, LANES), LANES)]
        high = value.astype(jnp.bfloat16).astype(jnp.float32)
        rest = value - high
        mid = rest.astype(jnp.bfloat16).astype(jnp.float32)
        low = rest - mid
        parts = jnp.concatenate([high, mid, low], axis=0).astype(jnp.bfloat16)
        chosen = jnp.where(rank == place_ref[pl.ds(b, 1), :], 1.0, 0.0).astype(jnp.bfloat16)
        ordered = lax.dot_general(parts, chosen, (((1,), (1,)), ((), ())), preferred_element_type=jnp.float32)
        return (ordered[0:rows] + ordered[rows : 2 * rows]) + ordered[2 * rows : 3 * rows]

    def pencil(b, ordered, s, ahead):
        base, count = base_ref[b, s], count_ref[b, s]
        start = base & (LANES - 1)
        end = start + count
        turned = pltpu.roll(ordered, (start - ahead) & (LANES - 1), 1)
        now = current[s] + jnp.where((lane >= start) & (lane < end), turned, 0.0)
        group = pl.multiple_of(base - start, LANES)
        after = jnp.where(lane < end - LANES, turned, 0.0)
        current[s] = jnp.where(end >= LANES, after, now)
        out_ref[s, :, pl.ds(group, 2 * LANES)] = jnp.concatenate([now, after], axis=1)
        return ahead + count

    n_blocks = planes * groups
    batch = 8 if n_blocks % 8 == 0 and n_tile <= 16 else 1

    def blocks(i, _):
        ordered = [sort(i * batch + j) for j in range(batch)]
        for j in range(batch):
            b = i * batch + j
            if n_tile <= 16:
                ahead = jnp.int32(0)
                for s in range(n_tile):
                    ahead = pencil(b, ordered[j], s, ahead)
            else:
                lax.fori_loop(0, n_tile, lambda s, ahead: pencil(b, ordered[j], s, ahead), jnp.int32(0))
        return 0

    lax.fori_loop(0, n_blocks // batch, blocks, 0)


def record_kernel(n_tile, chunks, sent_ref, matrix_ref, out_ref, got, records, send_sem, recv_sem, rsend_sem, rrecv_sem):
    g, t = lax.axis_index("grp"), lax.axis_index("tile")
    rows, nx, cap = sent_ref.shape[1], out_ref.shape[0], out_ref.shape[1]
    width = cap // chunks

    barrier = pltpu.get_barrier_semaphore()

    @pl.when(g < 3)
    def _():
        for k in range(1, n_tile):
            pl.semaphore_signal(barrier, inc=1, device_id=(g, lax.rem(t + k, n_tile)), device_id_type=MESH)
        pl.semaphore_signal(barrier, inc=1, device_id=(3, t), device_id_type=MESH)
        pl.semaphore_wait(barrier, n_tile)

    @pl.when(g == 3)
    def _():
        for k in range(3):
            pl.semaphore_signal(barrier, inc=1, device_id=(k, t), device_id_type=MESH)
        pl.semaphore_wait(barrier, 3)

    def exchange(s, slot, c):
        part = pl.ds(c * width, width)
        return pltpu.make_async_remote_copy(
            src_ref=sent_ref.at[s, :, part], dst_ref=got.at[slot, :, part], send_sem=send_sem.at[s, c],
            recv_sem=recv_sem.at[slot, c], device_id=(g, s), device_id_type=MESH)

    def report(c, slot):
        part = pl.ds(c * width, width)
        return pltpu.make_async_remote_copy(
            src_ref=out_ref.at[:, part], dst_ref=records.at[slot, :, part], send_sem=rsend_sem.at[c],
            recv_sem=rrecv_sem.at[slot, c], device_id=(3, t), device_id_type=MESH)

    @pl.when(g < 3)
    def _():
        for c in range(chunks):
            for k in range(1, n_tile):
                exchange(lax.rem(t + k, n_tile), t, c).start()
        got[t] = sent_ref[t, :, 0:cap]
        matrix = matrix_ref[...]
        for c in range(chunks):
            for k in range(1, n_tile):
                exchange(lax.rem(t + k, n_tile), lax.rem(t + k, n_tile), c).wait_recv()
            value = got[:, :, c * width : (c + 1) * width].reshape(nx, width)
            out_ref[:, c * width : (c + 1) * width] = jnp.dot(
                matrix, value, precision=lax.Precision.HIGHEST, preferred_element_type=jnp.float32)
            report(c, g).start()
        for c in range(chunks):
            for k in range(1, n_tile):
                exchange(lax.rem(t + k, n_tile), t, c).wait_send()
            report(c, g).wait_send()

    @pl.when(g == 3)
    def _():
        for c in range(chunks):
            for k in range(3):
                report(c, k).wait_recv()
            part = slice(c * width, (c + 1) * width)
            first, second, third = records[0, :, part], records[1, :, part], records[2, :, part]
            out_ref[:, part] = first * first + second * second + third * third


def body(flow_state, line_owner, *, n_tile):
    _, planes, rows, ny = flow_state.shape
    n_lines = line_owner.shape[0]
    n_blocks = n_lines // LANES
    nx = rows * n_tile
    cap = 2 * planes * ny // n_tile
    vmem = pl.BlockSpec(memory_space=pltpu.VMEM)
    smem = pl.BlockSpec(memory_space=pltpu.SMEM)
    f32 = jnp.float32
    shape = jax.ShapeDtypeStruct
    limit = 16 * 1024 * 1024
    dma = pltpu.SemaphoreType.DMA
    owner = line_owner.reshape(n_blocks, LANES)
    tile = (planes, rows, ny)
    ints = shape((n_blocks, LANES), jnp.int32)
    coeffs, place, base, count = pl.pallas_call(
        functools.partial(flow_kernel, n_tile),
        out_shape=(shape(tile, f32), shape((n_blocks, LANES), f32), ints, ints),
        in_specs=[vmem, vmem], out_specs=(vmem, vmem, vmem, vmem),
        scratch_shapes=[
            pltpu.VMEM((4,) + tile, f32), pltpu.VMEM((3,) + tile, f32),
            pltpu.VMEM((4,) + tile, f32), pltpu.VMEM((2,) + tile, f32),
            pltpu.VMEM((planes, rows + 2 * reach, ny), f32), pltpu.VMEM((planes, rows + 2 * reach, ny), f32),
            pltpu.VMEM(tile, f32), pltpu.VMEM(tile, f32), pltpu.VMEM(tile, f32), pltpu.VMEM(tile, f32), pltpu.VMEM(tile, f32),
            dma((4,)), dma((4, 2)), dma((2,)), dma((4,)), dma((4,)), dma((4,)), dma((2,)), dma((2,)), dma((4,)),
            pltpu.VMEM((4 * LANES, 2 * LANES), f32),
        ],
        compiler_params=pltpu.CompilerParams(has_side_effects=True, collective_id=0, vmem_limit_bytes=limit), name="flow",
    )(flow_state, owner)
    sent = pl.pallas_call(
        functools.partial(compact_kernel, n_tile),
        out_shape=shape((n_tile, rows, cap + 2 * LANES), f32),
        in_specs=[smem, smem, vmem, vmem], out_specs=vmem,
        scratch_shapes=[pltpu.VMEM((n_tile, rows, LANES), f32)],
        compiler_params=pltpu.CompilerParams(vmem_limit_bytes=limit), name="compact",
    )(base, count, coeffs, place)
    chunks = 4 if cap % (4 * LANES) == 0 else 1
    record = pl.pallas_call(
        functools.partial(record_kernel, n_tile, chunks),
        out_shape=shape((nx, cap), f32),
        in_specs=[vmem, vmem], out_specs=vmem,
        scratch_shapes=[
            pltpu.VMEM((n_tile, rows, cap), f32), pltpu.VMEM((3, nx, cap), f32),
            dma((n_tile, chunks)), dma((n_tile, chunks)), dma((chunks,)), dma((3, chunks)),
        ],
        compiler_params=pltpu.CompilerParams(has_side_effects=True, collective_id=1, vmem_limit_bytes=limit), name="record",
    )(sent, jnp.asarray(lift_matrix(nx).astype(np.float32)))
    return record[None, None]


def solution(mesh):
    in_specs = (P("grp", None, "tile", None), P())
    out_specs = P("grp", "tile", None, None)
    run = functools.partial(body, n_tile=mesh.shape["tile"])
    return jax.shard_map(run, mesh=mesh, in_specs=in_specs, out_specs=out_specs, check_vma=False)
```
